16 devices in a mesh: dp: 2 (over y, z), fsdp: 8 (over x, core).
Axes of the slice: x: 4, y: 2, z: 1, core: 2. Of those that a mesh axis runs over, the one named last changes fastest.
The devices are a block of a 4x4x8 slice.
Arguments:
- hidden: bfloat16 [48, 768, 2048], P(('dp', 'fsdp')), parts along dimension 0
- g_attn: bfloat16 [2048], P('fsdp')
- w_query: bfloat16 [2048, 2048], P('fsdp')
- w_key: bfloat16 [2048, 256], P('fsdp')
- w_value: bfloat16 [2048, 256], P('fsdp')
- w_out: bfloat16 [2048, 2048], P('fsdp')
- g_mlp: bfloat16 [2048], P('fsdp')
- w_gate: bfloat16 [2048, 11008], P('fsdp')
- w_up: bfloat16 [2048, 11008], P('fsdp')
- w_down: bfloat16 [11008, 2048], P('fsdp')
- cos_tab: float32 [768, 64], replicated
- sin_tab: float32 [768, 64], replicated
Outputs:
- output 1: bfloat16 [48, 768, 2048], P(('dp', 'fsdp')), parts along dimension 0
- output 2: bfloat16 [48, 768, 2, 128], P(('dp', 'fsdp')), parts along dimension 0
- output 3: bfloat16 [48, 768, 2, 128], P(('dp', 'fsdp')), parts along dimension 0
There are 2 independent parts. The reference program is written for one: setup_inputs(seed, part) draws one part's arguments, and reference() takes and returns one part's arrays. A program takes and returns all parts, laid end to end along the dimension named above; an argument that names none is the same for every part.
All inputs are finite; a program needn't handle non-finite values.
Results may differ from the reference program's by a relative error of at most 0.0191086.
Values are sent between devices in bfloat16 or wider.
A program may use at most 768 MiB of HBM per device.

```python
import jax
import jax.numpy as jnp
from jax import lax

BATCH_ROWS = 24
SEQ_LEN = 768
MODEL_DIM = 2048
NUM_HEADS = 16
KV_HEADS = 2
HEAD_DIM = 128
FFN_DIM = 11008
QUERY_BLOCK = 256
ROPE_BASE = 500000.0
NORM_EPS = 1e-5


def make_weight(rng_key, fan_in, fan_out, factor):
    normal_draw = jax.random.normal(rng_key, (fan_in, fan_out), jnp.float32)
    return (normal_draw * (factor * fan_in ** -0.5)).astype(jnp.bfloat16)


def make_gain(rng_key):
    return jax.random.uniform(rng_key, (MODEL_DIM,), jnp.float32, 0.5, 1.5).astype(jnp.bfloat16)


def rope_tables(rng_key):
    start_pos = jax.random.randint(rng_key, (), 0, 8192)
    inv_freq = 1.0 / (ROPE_BASE ** (jnp.arange(0, HEAD_DIM, 2).astype(jnp.float32) / HEAD_DIM))
    positions = (start_pos + jnp.arange(SEQ_LEN)).astype(jnp.float32)
    angles = positions[:, None] * inv_freq[None, :]
    return jnp.cos(angles), jnp.sin(angles)


def setup_inputs(seed: int = 0, part: int = 0) -> dict:
    sub_keys = jax.random.split(jax.random.key(seed), 11)
    part_key = jax.random.fold_in(sub_keys[0], part)
    q_width = NUM_HEADS * HEAD_DIM
    kv_width = KV_HEADS * HEAD_DIM
    hidden = 0.5 * jax.random.normal(part_key, (BATCH_ROWS, SEQ_LEN, MODEL_DIM), jnp.float32)
    cos_tab, sin_tab = rope_tables(sub_keys[10])
    return {
        "hidden": hidden.astype(jnp.bfloat16),
        "g_attn": make_gain(sub_keys[1]),
        "w_query": make_weight(sub_keys[2], MODEL_DIM, q_width, 2.0),
        "w_key": make_weight(sub_keys[3], MODEL_DIM, kv_width, 1.0),
        "w_value": make_weight(sub_keys[4], MODEL_DIM, kv_width, 1.0),
        "w_out": make_weight(sub_keys[5], q_width, MODEL_DIM, 1.0),
        "g_mlp": make_gain(sub_keys[6]),
        "w_gate": make_weight(sub_keys[7], MODEL_DIM, FFN_DIM, 1.0),
        "w_up": make_weight(sub_keys[8], MODEL_DIM, FFN_DIM, 1.0),
        "w_down": make_weight(sub_keys[9], FFN_DIM, MODEL_DIM, 1.0),
        "cos_tab": cos_tab,
        "sin_tab": sin_tab,
    }


def rms_norm(rows_in, gain_vec):
    upcast = rows_in.astype(jnp.float32)
    scaled = upcast * lax.rsqrt(jnp.mean(upcast * upcast, axis=-1, keepdims=True) + NORM_EPS)
    return (scaled * gain_vec.astype(jnp.float32)).astype(jnp.bfloat16)


def apply_rope(heads_in, cos_tab, sin_tab):
    half_dim = HEAD_DIM // 2
    upcast = heads_in.astype(jnp.float32)
    lo_half = upcast[..., :half_dim]
    hi_half = upcast[..., half_dim:]
    cos_bc = cos_tab[:, None, :]
    sin_bc = sin_tab[:, None, :]
    rotated = jnp.concatenate([lo_half * cos_bc - hi_half * sin_bc, hi_half * cos_bc + lo_half * sin_bc], axis=-1)
    return rotated.astype(jnp.bfloat16)


def reference(hidden, g_attn, w_query, w_key, w_value, w_out, g_mlp, w_gate, w_up, w_down, cos_tab, sin_tab):
    group_size = NUM_HEADS // KV_HEADS
    key_pos = jnp.arange(SEQ_LEN)

    def one_sequence(seq_in):
        normed = rms_norm(seq_in, g_attn)
        query_proj = jnp.dot(normed, w_query, preferred_element_type=jnp.float32).astype(jnp.bfloat16)
        key_proj = jnp.dot(normed, w_key, preferred_element_type=jnp.float32).astype(jnp.bfloat16)
        value_proj = jnp.dot(normed, w_value, preferred_element_type=jnp.float32).astype(jnp.bfloat16)
        query_rot = apply_rope(query_proj.reshape(SEQ_LEN, NUM_HEADS, HEAD_DIM), cos_tab, sin_tab)
        key_rot = apply_rope(key_proj.reshape(SEQ_LEN, KV_HEADS, HEAD_DIM), cos_tab, sin_tab)
        value_heads = value_proj.reshape(SEQ_LEN, KV_HEADS, HEAD_DIM)
        query_grp = query_rot.reshape(SEQ_LEN, KV_HEADS, group_size, HEAD_DIM).astype(jnp.float32)
        key_wide = key_rot.astype(jnp.float32)
        value_wide = value_heads.astype(jnp.float32)

        def one_block(block_idx):
            blk_start = block_idx * QUERY_BLOCK
            query_blk = lax.dynamic_slice_in_dim(query_grp, blk_start, QUERY_BLOCK, axis=0)
            scores = jnp.einsum("qkgd,skd->kgqs", query_blk, key_wide) * HEAD_DIM ** -0.5
            query_pos = blk_start + jnp.arange(QUERY_BLOCK)
            scores = jnp.where(key_pos[None, :] <= query_pos[:, None], scores, -jnp.inf)
            prob_bf16 = jax.nn.softmax(scores, axis=-1).astype(jnp.bfloat16)
            mixed_vals = jnp.einsum("kgqs,skd->qkgd", prob_bf16.astype(jnp.float32), value_wide)
            return mixed_vals.astype(jnp.bfloat16)

        attn_heads = lax.map(one_block, jnp.arange(SEQ_LEN // QUERY_BLOCK))
        attn_flat = attn_heads.reshape(SEQ_LEN, NUM_HEADS * HEAD_DIM)
        attn_proj = jnp.dot(attn_flat, w_out, preferred_element_type=jnp.float32).astype(jnp.bfloat16)
        residual = (seq_in.astype(jnp.float32) + attn_proj.astype(jnp.float32)).astype(jnp.bfloat16)
        normed_mlp = rms_norm(residual, g_mlp)
        gate_proj = jnp.dot(normed_mlp, w_gate, preferred_element_type=jnp.float32).astype(jnp.bfloat16)
        up_proj = jnp.dot(normed_mlp, w_up, preferred_element_type=jnp.float32).astype(jnp.bfloat16)
        act_in = (jax.nn.silu(gate_proj.astype(jnp.float32)) * up_proj.astype(jnp.float32)).astype(jnp.bfloat16)
        mlp_out = jnp.dot(act_in, w_down, preferred_element_type=jnp.float32).astype(jnp.bfloat16)
        out_seq = (residual.astype(jnp.float32) + mlp_out.astype(jnp.float32)).astype(jnp.bfloat16)
        return out_seq, key_rot, value_heads

    out_hidden, k_cache, v_cache = lax.map(one_sequence, hidden)
    return (out_hidden, k_cache, v_cache)
```

```python
import functools, math
import jax, jax.numpy as jnp
from jax import lax
from jax.experimental import pallas as pl
from jax.experimental.pallas import tpu as pltpu
from jax.sharding import PartitionSpec as P

F32 = jnp.float32
BF = jnp.bfloat16
MESH = pl.DeviceIdType.MESH
HBM = pltpu.MemorySpace.HBM
EPS = 1e-5


class Group:
    def __init__(self, name, local, col0, outer, common, rows, nblk):
        self.name, self.local, self.col0 = name, local, col0
        self.outer, self.common, self.rows, self.nblk = outer, common, rows, nblk
        self.width = 2 * outer + common

    def shape(self):
        return jax.ShapeDtypeStruct((self.rows * self.nblk, self.width), BF)


def place(nblk):
    me = lax.axis_index("fsdp")
    dp = lax.axis_index("dp")
    core = lax.rem(me, 2)
    chip = me // 2
    chips = nblk // 2
    par = lax.rem(dp, 2)
    blk = lambda k: lax.rem(chip + k, chips) * 2 + core
    return dict(me=me, par=par, core=core,
                left=blk(chips - 1), right=blk(1), far=blk(2), mate=me + 1 - 2 * core,
                dev_left=(dp, blk(chips - 1)), dev_right=(dp, blk(1)), dev_mate=(dp, me + 1 - 2 * core),
                dev_pair=(dp + 1 - 2 * par, me))


def stage_copies(g, stage, at, loc, full):
    R, H, m, mc = g.rows, g.rows // 2, g.outer, g.outer + g.common
    par = at["par"]
    cols = lambda start, n: pl.ds(pl.multiple_of(start, 128), n)
    rows = lambda b, o=0, n=R: pl.ds(pl.multiple_of(b * R + o, 16), n)
    xr, mine, theirs = cols(par * m, mc), cols(par * mc, m), cols((1 - par) * mc, m)
    if stage == 1:
        src = loc.at[:, cols(g.col0 + par * m, mc)]
        own = rows(at["me"])
        return [(src, full.at[own, xr], at["dev_right"]), (src, full.at[own, xr], at["dev_left"]),
                (loc.at[:, pl.ds(g.col0, g.width)], full.at[own, :], at["dev_mate"])]
    same = lambda r, c, dev: (full.at[r, c], full.at[r, c], dev)
    lo, hi, far, mate = at["left"], at["right"], at["far"], at["mate"]
    allc = pl.ds(0, g.width)
    if stage == 2:
        out = [same(rows(lo, 0, H), xr, at["dev_right"]), same(rows(hi, H, H), xr, at["dev_left"])]
        if m:
            out += [same(rows(lo), mine, at["dev_pair"]), same(rows(hi), mine, at["dev_pair"])]
        return out + [same(rows(lo), xr, at["dev_mate"]), same(rows(hi), xr, at["dev_mate"]), same(rows(mate), allc, at["dev_mate"])]
    if stage == 3:
        out = []
        if m:
            out += [same(rows(far), mine, at["dev_pair"])]
        out += [same(rows(far), xr, at["dev_mate"])]
        if m:
            out += [same(rows(lo), theirs, at["dev_mate"]), same(rows(hi), theirs, at["dev_mate"])]
        return out
    return [same(rows(far), theirs, at["dev_mate"])] if m else []


def n_copies(g, stage):
    m = g.outer > 0
    return {1: 3, 2: 7 if m else 5, 3: 4 if m else 1, 4: 1 if m else 0}[stage]


def call(name, cid, body, grid, ins, in_specs, outs, out_specs, ticks, bufs, locs, nblk, flops=0, nbytes=0, scratch=(), alias=None):
    groups = []
    for _, acts in ticks:
        for g, s in acts:
            if g not in groups:
                groups.append(g)
    old = [g for g in groups if g.name in bufs]
    new = [g for g in groups if g.name not in bufs]
    lnames = []
    for _, acts in ticks:
        for g, s in acts:
            if s == 1 and g.local not in lnames:
                lnames.append(g.local)
    base, total = {}, 0
    for _, acts in ticks:
        for g, s in acts:
            base[(g.name, s)] = total
            total += n_copies(g, s)
    nsteps = math.prod(grid)
    n_in, n_out, n_sc = len(ins), len(outs), len(scratch)

    def kernel(*refs):
        cin, refs = refs[:n_in], refs[n_in:]
        lrefs, refs = refs[:len(lnames)], refs[len(lnames):]
        refs = refs[len(old):]
        couts, refs = refs[:n_out], refs[n_out:]
        gref, refs = refs[:len(groups)], refs[len(groups):]
        sc, refs = refs[:n_sc], refs[n_sc:]
        if not total:
            body(cin, couts, sc)
            return
        ssem, rsem = refs
        full = {g.name: r for g, r in zip(old + new, gref)}
        loc = dict(zip(lnames, lrefs))
        step = pl.program_id(0)
        for k in range(1, len(grid)):
            step = step * grid[k] + pl.program_id(k)
        at = place(nblk)

        def copies(g, s):
            b = base[(g.name, s)]
            return [pltpu.make_async_remote_copy(src_ref=a, dst_ref=d, send_sem=ssem.at[b + k], recv_sem=rsem.at[b + k],
                                                 device_id=dev, device_id_type=MESH)
                    for k, (a, d, dev) in enumerate(stage_copies(g, s, at, loc.get(g.local), full[g.name]))]

        got = set()
        for n, (when, acts) in enumerate(ticks):
            need = []
            for g, s in acts:
                if (g.name, s - 1) in base and (g.name, s - 1) not in got:
                    need.append((g, s - 1))
                    got.add((g.name, s - 1))

            @pl.when(step == when)
            def _():
                if n == 0:
                    bar = pltpu.get_barrier_semaphore()
                    for dev in ("dev_left", "dev_right", "dev_mate", "dev_pair"):
                        pl.semaphore_signal(bar, inc=1, device_id=at[dev], device_id_type=MESH)
                    pl.semaphore_wait(bar, 4)
                for g, s in need:
                    for cp in copies(g, s):
                        cp.wait_recv()
                for g, s in acts:
                    for cp in copies(g, s):
                        cp.start()

        body(cin, couts, sc)

        @pl.when(step == nsteps - 1)
        def _():
            for _, acts in ticks:
                for g, s in acts:
                    for cp in copies(g, s):
                        if (g.name, s) not in got:
                            cp.wait_recv()
                        cp.wait_send()

    hb = pl.BlockSpec(memory_space=HBM)
    al = dict(alias or {})
    for k in range(len(old)):
        al[n_in + len(lnames) + k] = n_out + k
    res = pl.pallas_call(
        kernel, grid=grid,
        in_specs=list(in_specs) + [hb] * (len(lnames) + len(old)),
        out_specs=list(out_specs) + [hb] * len(groups),
        out_shape=list(outs) + [g.shape() for g in old + new],
        scratch_shapes=list(scratch) + ([pltpu.SemaphoreType.DMA((total,)), pltpu.SemaphoreType.DMA((total,))] if total else []),
        input_output_aliases=al,
        compiler_params=pltpu.CompilerParams(vmem_limit_bytes=62 << 20, **(dict(collective_id=cid, has_side_effects=True) if total else {})),
        cost_estimate=pl.CostEstimate(flops=flops, bytes_accessed=nbytes, transcendentals=0),
        name=name)(*ins, *[locs[n] for n in lnames], *[bufs[g.name] for g in old])
    for g, b in zip(old + new, res[n_out:]):
        bufs[g.name] = b
    return res[:n_out]


def norm_body(cin, couts, sc):
    x_ref, g_ref = cin
    x = x_ref[...].astype(F32)
    r = lax.rsqrt(jnp.mean(x * x, axis=-1, keepdims=True) + EPS)
    couts[0][...] = (x * r * g_ref[...].astype(F32)).astype(BF)


def qkv_body(qw, kw, cin, couts, sc):
    h_ref, *w_refs, cos_ref, sin_ref = cin
    q_ref, k_ref, v_ref = couts
    hd = cos_ref.shape[1]
    c, s = cos_ref[...], sin_ref[...]
    col = 0
    for w_ref in w_refs:
        for n0 in range(0, w_ref.shape[1], 2 * hd):
            acc = jnp.dot(h_ref[...], w_ref[:, n0:n0 + 2 * hd], preferred_element_type=F32).astype(BF)
            for j in (0, hd):
                part = acc[:, j:j + hd]
                if col < qw + kw:
                    t = part.astype(F32)
                    part = (t * c + pltpu.roll(t, hd // 2, 1) * s).astype(BF)
                if col < qw:
                    q_ref[:, col:col + hd] = part
                elif col < qw + kw:
                    k_ref[:, col - qw:col - qw + hd] = part
                else:
                    v_ref[:, col - qw - kw:col - qw - kw + hd] = part
                col += hd


def attn_body(hd, qb, unroll, cin, couts, sc):
    q_ref, k_ref, v_ref = cin
    o_ref, = couts
    S, nh = q_ref.shape[0], q_ref.shape[1] // hd
    scale = hd ** -0.5 * math.log2(math.e)
    mask = lax.broadcasted_iota(jnp.int32, (qb, qb), 0) >= lax.broadcasted_iota(jnp.int32, (qb, qb), 1)

    def one(head):
        hs = pl.ds(pl.multiple_of(head * hd, hd), hd)
        for b in range(S // qb):
            n = (b + 1) * qb
            qq = q_ref[b * qb:n, hs]
            s = lax.dot_general(qq, k_ref[:n, :], (((1,), (1,)), ((), ())), preferred_element_type=F32)
            diag = jnp.where(mask, s[:, b * qb:], -jnp.inf)
            s = diag if b == 0 else jnp.concatenate([s[:, :b * qb], diag], axis=1)
            p = jnp.exp2((s - jnp.max(s, axis=1, keepdims=True)) * scale)
            pb = (p * (1.0 / jnp.sum(p, axis=1, keepdims=True))).astype(BF)
            o_ref[b * qb:n, hs] = jnp.dot(pb, v_ref[:n, :], preferred_element_type=F32).astype(BF)

    def step(i, _):
        for u in range(unroll):
            one(i * unroll + u)
        return 0
    lax.fori_loop(0, nh // unroll, step, 0)


def wout_body(cin, couts, sc):
    *o_refs, w_ref, x_ref, g_ref = cin
    x1_ref, h_ref = couts
    D = w_ref.shape[1]
    o = jnp.concatenate([r[...] for r in o_refs], axis=1)
    ss = jnp.zeros((o.shape[0], 1), F32)
    step = min(512, D)
    for n0 in range(0, D, step):
        cs = slice(n0, n0 + step)
        a = jnp.dot(o, w_ref[:, cs], preferred_element_type=F32).astype(BF)
        x1 = (x_ref[:, cs].astype(F32) + a.astype(F32)).astype(BF)
        x1_ref[:, cs] = x1
        xf = x1.astype(F32)
        ss = ss + jnp.sum(xf * xf, axis=1, keepdims=True)
    r = lax.rsqrt(ss / D + EPS)
    for n0 in range(0, D, step):
        cs = slice(n0, n0 + step)
        h_ref[:, cs] = (x1_ref[:, cs].astype(F32) * r * g_ref[:, cs].astype(F32)).astype(BF)


def gu_body(mt, cin, couts, sc):
    h_ref, wg_ref, wu_ref = cin[:3]
    r_ref, = couts

    def step(i, _):
        rs = pl.ds(pl.multiple_of(i * mt, mt), mt)
        hh = h_ref[rs, :]
        g = jnp.dot(hh, wg_ref[...], preferred_element_type=F32).astype(BF).astype(F32)
        u = jnp.dot(hh, wu_ref[...], preferred_element_type=F32).astype(BF).astype(F32)
        r_ref[rs, :] = ((g / (1.0 + jnp.exp(-g))) * u).astype(BF)
        return 0
    lax.fori_loop(0, h_ref.shape[0] // mt, step, 0)


def down_body(cin, couts, sc):
    r_ref, w_ref, x_ref = cin[:3]
    m = jnp.dot(r_ref[...], w_ref[...], preferred_element_type=F32).astype(BF)
    couts[0][...] = (x_ref[...].astype(F32) + m.astype(F32)).astype(BF)


UNIT = 256
GU_UNITS = (6, 6, 6, 6, 6, 6, 7)
DOWN_COLS = (512, 512, 512, 512)


def thirds(cols, unit, frac=1 / 3):
    outer = int(cols // unit * frac + 0.5) * unit
    return outer, cols - 2 * outer


def local_layer(nblk, hidden, g_attn, w_query, w_key, w_value, w_out, g_mlp, w_gate, w_up, w_down, cos_tab, sin_tab):
    B, S, D = hidden.shape
    T = B * S
    hd = 2 * cos_tab.shape[1]
    qw, kw = w_query.shape[1], w_key.shape[1]
    ff = w_gate.shape[1]
    kv = kw // hd
    x = hidden.reshape(T, D)
    gains = lax.all_gather(jnp.stack([g_attn, g_mlp]), "fsdp", axis=1, tiled=True)
    ga, gm = gains[0:1], gains[1:2]
    cos2 = jnp.concatenate([cos_tab, cos_tab], axis=1)
    sin2 = jnp.concatenate([-sin_tab, sin_tab], axis=1)
    locs = dict(wq=jnp.concatenate([w_query, w_key, w_value], axis=1), wo=w_out, wg=w_gate, wu=w_up, wd=w_down)
    rw = w_query.shape[0]
    qk = qw + 2 * kw
    half = qk // 2
    Q = [Group("q%d" % k, "wq", k * half, *thirds(half, 128, .2), rw, nblk) for k in range(2)]
    WO = Group("wo", "wo", 0, *thirds(D, 128), rw, nblk)
    G, c0 = [], 0
    for k, u in enumerate(GU_UNITS):
        G.append([Group("g%d" % k, "wg", c0, *thirds(u * UNIT, 128), rw, nblk), Group("u%d" % k, "wu", c0, *thirds(u * UNIT, 128), rw, nblk)])
        c0 += u * UNIT
    assert c0 == ff
    Dn, c0 = [], 0
    for k, w in enumerate(DOWN_COLS):
        Dn.append(Group("d%d" % k, "wd", c0, *thirds(w, 128), w_down.shape[0], nblk))
        c0 += w
    assert c0 == D
    seq = [[g] if isinstance(g, Group) else g for g in G + Dn]

    def acts(i):
        out = []
        for s in (2, 3, 4, 1):
            if 0 <= i - (s - 1) < len(seq):
                out += [(g, s) for g in seq[i - (s - 1)] if n_copies(g, s)]
        return out

    bufs = {}
    run = functools.partial(call, bufs=bufs, locs=locs, nblk=nblk)
    sd = jax.ShapeDtypeStruct
    mt = 256
    row = lambda i: (i, 0)
    const = lambda *a: (0, 0)
    cid = 0
    h, = run("gather_norm", cid, norm_body, (T // mt,), [x, ga], [pl.BlockSpec((mt, D), row), pl.BlockSpec((1, D), const)],
             [sd((T, D), BF)], [pl.BlockSpec((mt, D), row)],
             [(0, [(Q[0], 1), (Q[1], 1)]), (1, [(Q[0], 2)]), (2, [(Q[1], 2)]), (3, [(WO, 1)]), (4, [(Q[0], 3)]), (5, [(Q[1], 3)]), (6, [(Q[0], 4), (Q[1], 4)])])
    tab = pl.BlockSpec((mt, hd), lambda i: (i % (S // mt), 0))
    cid += 1
    q, k, v = run("qkv", cid, functools.partial(qkv_body, qw, kw), (T // mt,), [h, bufs["q0"], bufs["q1"], cos2, sin2],
                  [pl.BlockSpec((mt, D), row)] + [pl.BlockSpec((D, half), const)] * 2 + [tab, tab],
                  [sd((T, qw), BF), sd((T, kw), BF), sd((T, kw), BF)],
                  [pl.BlockSpec((mt, qw), row), pl.BlockSpec((mt, kw), row), pl.BlockSpec((mt, kw), row)],
                  [(0, [(WO, 2)] + acts(0))], flops=2 * T * D * qk, nbytes=4 * T * D)
    o = []
    for j in range(kv):
        cid += 1
        gw = qw // kv
        o += run("attn%d" % j, cid, functools.partial(attn_body, hd, 256, 4), (B,), [q, k, v],
                 [pl.BlockSpec((S, gw), lambda b, j=j: (b, j)), pl.BlockSpec((S, hd), lambda b, j=j: (b, j)), pl.BlockSpec((S, hd), lambda b, j=j: (b, j))],
                 [sd((T, gw), BF)], [pl.BlockSpec((S, gw), row)],
                 [(0, [(WO, 3 + j)] + acts(1 + j))], flops=T * S * gw * 8, nbytes=4 * T * gw)
    cid += 1
    x1, h2 = run("wout", cid, wout_body, (T // mt,), o + [bufs["wo"], x, gm],
                 [pl.BlockSpec((mt, qw // kv), row)] * kv + [pl.BlockSpec((qw, D), const), pl.BlockSpec((mt, D), row), pl.BlockSpec((1, D), const)],
                 [sd((T, D), BF)] * 2, [pl.BlockSpec((mt, D), row)] * 2, [(0, acts(3))], flops=2 * T * D * qw, nbytes=8 * T * D)
    r, n0 = None, 0
    mtg = 768
    for j, u in enumerate(GU_UNITS):
        cid += 1
        ins = [h2, bufs["g%d" % j], bufs["u%d" % j]] + ([r] if r is not None else [])
        specs = [pl.BlockSpec((mtg, D), lambda n, i: (i, 0)), pl.BlockSpec((D, UNIT), lambda n, i: (0, n)), pl.BlockSpec((D, UNIT), lambda n, i: (0, n))]
        specs += [pl.BlockSpec(memory_space=HBM)] if r is not None else []
        r, = run("gateup%d" % j, cid, functools.partial(gu_body, mtg), (u, T // mtg), ins, specs,
                 [sd((T, ff), BF)], [pl.BlockSpec((mtg, UNIT), lambda n, i, n0=n0: (i, n0 + n))],
                 [(0, acts(4 + j))], flops=4 * T * D * UNIT * u, nbytes=4 * T * D, alias={3: 0} if r is not None else None)
        n0 += u
    out, c0 = None, 0
    for j, w in enumerate(DOWN_COLS):
        cid += 1
        ins = [r, bufs["d%d" % j], x1] + ([out] if out is not None else [])
        off = c0 // w
        specs = [pl.BlockSpec((mt, ff), row), pl.BlockSpec((ff, w), const), pl.BlockSpec((mt, w), lambda i, off=off: (i, off))]
        specs += [pl.BlockSpec(memory_space=HBM)] if out is not None else []
        a = acts(4 + len(GU_UNITS) + j)
        out, = run("down%d" % j, cid, down_body, (T // mt,), ins, specs, [sd((T, D), BF)], [pl.BlockSpec((mt, w), lambda i, off=off: (i, off))],
                   [(0, a)] if a else [], flops=2 * T * ff * w, nbytes=2 * T * ff, alias={3: 0} if out is not None else None)
        c0 += w
    return out.reshape(B, S, D), k.reshape(B, S, kv, hd), v.reshape(B, S, kv, hd)


def solution(mesh):
    tok = P(("dp", "fsdp"), None, None)
    cache = P(("dp", "fsdp"), None, None, None)
    rowp, gain, table = P("fsdp", None), P("fsdp"), P(None, None)
    return jax.shard_map(functools.partial(local_layer, mesh.shape["fsdp"]), mesh=mesh,
                         in_specs=(tok, gain, rowp, rowp, rowp, rowp, gain, rowp, rowp, rowp, table, table),
                         out_specs=(tok, cache, cache), check_vma=False)
```

```python
import functools, math
import jax, jax.numpy as jnp
from jax import lax
from jax.experimental import pallas as pl
from jax.experimental.pallas import tpu as pltpu
from jax.sharding import PartitionSpec as P

F32 = jnp.float32
BF = jnp.bfloat16
MESH = pl.DeviceIdType.MESH
HBM = pltpu.MemorySpace.HBM
EPS = 1e-5


class Group:
    def __init__(self, name, local, col0, outer, common, rows, nblk):
        self.name, self.local, self.col0 = name, local, col0
        self.outer, self.common, self.rows, self.nblk = outer, common, rows, nblk
        self.width = 2 * outer + common

    def shape(self):
        return jax.ShapeDtypeStruct((self.rows * self.nblk, self.width), BF)


def place(nblk):
    me = lax.axis_index("fsdp")
    dp = lax.axis_index("dp")
    core = lax.rem(me, 2)
    chip = me // 2
    chips = nblk // 2
    par = lax.rem(dp, 2)
    blk = lambda k: lax.rem(chip + k, chips) * 2 + core
    return dict(me=me, dp=dp, par=par, core=core,
                left=blk(chips - 1), right=blk(1), far=blk(2), mate=me + 1 - 2 * core,
                dev_left=(dp, blk(chips - 1)), dev_right=(dp, blk(1)), dev_mate=(dp, me + 1 - 2 * core),
                dev_pair=(dp + 1 - 2 * par, me))


def stage_copies(g, stage, at, loc, full):
    R, H, m, mc = g.rows, g.rows // 2, g.outer, g.outer + g.common
    par = at["par"]
    cols = lambda start, n: pl.ds(pl.multiple_of(start, 128), n)
    rows = lambda b, o=0, n=R: pl.ds(pl.multiple_of(b * R + o, 16), n)
    xr, mine, theirs = cols(par * m, mc), cols(par * mc, m), cols((1 - par) * mc, m)
    if stage == 1:
        src = loc.at[:, cols(g.col0 + par * m, mc)]
        own = rows(at["me"])
        return [(src, full.at[own, xr], at["dev_right"]), (src, full.at[own, xr], at["dev_left"]),
                (loc.at[:, pl.ds(g.col0, g.width)], full.at[own, :], at["dev_mate"])]
    same = lambda r, c, dev: (full.at[r, c], full.at[r, c], dev)
    lo, hi, far, mate = at["left"], at["right"], at["far"], at["mate"]
    allc = pl.ds(0, g.width)
    if stage == 2:
        out = [same(rows(lo, 0, H), xr, at["dev_right"]), same(rows(hi, H, H), xr, at["dev_left"])]
        if m:
            out += [same(rows(lo), mine, at["dev_pair"]), same(rows(hi), mine, at["dev_pair"])]
        return out + [same(rows(lo), xr, at["dev_mate"]), same(rows(hi), xr, at["dev_mate"]), same(rows(mate), allc, at["dev_mate"])]
    if stage == 3:
        out = []
        if m:
            out += [same(rows(far), mine, at["dev_pair"])]
        out += [same(rows(far), xr, at["dev_mate"])]
        if m:
            out += [same(rows(lo), theirs, at["dev_mate"]), same(rows(hi), theirs, at["dev_mate"])]
        return out
    return [same(rows(far), theirs, at["dev_mate"])] if m else []


def n_copies(g, stage):
    m = g.outer > 0
    return {1: 3, 2: 7 if m else 5, 3: 4 if m else 1, 4: 1 if m else 0}[stage]


def call(name, cid, body, grid, ins, in_specs, outs, out_specs, ticks, bufs, locs, nblk, flops=0, nbytes=0, scratch=(), alias=None, pre=None, everyone=False, held=()):
    groups = []
    for _, acts in ticks:
        for g, s in acts:
            if g not in groups:
                groups.append(g)
    old = [g for g in groups if g.name in bufs]
    new = [g for g in groups if g.name not in bufs]
    lnames = []
    for _, acts in ticks:
        for g, s in acts:
            if s == 1 and g.local not in lnames:
                lnames.append(g.local)
    base, total = {}, 0
    for _, acts in ticks:
        for g, s in acts:
            base[(g.name, s)] = total
            total += n_copies(g, s)
    nsteps = math.prod(grid)
    n_in, n_out, n_sc = len(ins), len(outs), len(scratch)
    in_specs = [pl.BlockSpec(memory_space=HBM) if k in held else sp for k, sp in enumerate(in_specs)]

    def kernel(*refs):
        cin, refs = refs[:n_in], refs[n_in:]
        lrefs, refs = refs[:len(lnames)], refs[len(lnames):]
        refs = refs[len(old):]
        couts, refs = refs[:n_out], refs[n_out:]
        gref, refs = refs[:len(groups)], refs[len(groups):]
        sc, refs = refs[:n_sc], refs[n_sc:]
        step = pl.program_id(0)
        for k in range(1, len(grid)):
            step = step * grid[k] + pl.program_id(k)
        if held:
            kept, hsem, refs = refs[:len(held)], refs[len(held)], refs[len(held) + 1:]
            loads = [pltpu.make_async_copy(cin[k], b, hsem.at[i]) for i, (k, b) in enumerate(zip(held, kept))]
            cin = list(cin)
            for k, b in zip(held, kept):
                cin[k] = b

            @pl.when(step == 0)
            def _():
                for cp in loads:
                    cp.start()

        def compute():
            if held:
                @pl.when(step == 0)
                def _():
                    for cp in loads:
                        cp.wait()
            body(cin, couts, sc)

        if not total:
            compute()
            return
        ssem, rsem = refs
        full = {g.name: r for g, r in zip(old + new, gref)}
        loc = dict(zip(lnames, lrefs))
        at = place(nblk)
        if pre is not None:
            pre(step, cin, sc)

        def copies(g, s):
            b = base[(g.name, s)]
            return [pltpu.make_async_remote_copy(src_ref=a, dst_ref=d, send_sem=ssem.at[b + k], recv_sem=rsem.at[b + k],
                                                 device_id=dev, device_id_type=MESH)
                    for k, (a, d, dev) in enumerate(stage_copies(g, s, at, loc.get(g.local), full[g.name]))]

        got = set()
        for n, (when, acts) in enumerate(ticks):
            need = []
            for g, s in acts:
                if (g.name, s - 1) in base and (g.name, s - 1) not in got:
                    need.append((g, s - 1))
                    got.add((g.name, s - 1))

            @pl.when(step == when)
            def _():
                if n == 0:
                    bar = pltpu.get_barrier_semaphore()
                    peers = [at[dev] for dev in ("dev_left", "dev_right", "dev_mate", "dev_pair")]
                    if everyone:
                        peers = [(at["dp"], lax.rem(at["me"] + j, nblk)) for j in range(1, nblk)] + [at["dev_pair"]]
                    for dev in peers:
                        pl.semaphore_signal(bar, inc=1, device_id=dev, device_id_type=MESH)
                    pl.semaphore_wait(bar, len(peers))
                for g, s in need:
                    for cp in copies(g, s):
                        cp.wait_recv()
                for g, s in acts:
                    for cp in copies(g, s):
                        cp.start()

        compute()

        @pl.when(step == nsteps - 1)
        def _():
            for _, acts in ticks:
                for g, s in acts:
                    for cp in copies(g, s):
                        if (g.name, s) not in got:
                            cp.wait_recv()
                        cp.wait_send()

    hb = pl.BlockSpec(memory_space=HBM)
    al = dict(alias or {})
    for k in range(len(old)):
        al[n_in + len(lnames) + k] = n_out + k
    res = pl.pallas_call(
        kernel, grid=grid,
        in_specs=list(in_specs) + [hb] * (len(lnames) + len(old)),
        out_specs=list(out_specs) + [hb] * len(groups),
        out_shape=list(outs) + [g.shape() for g in old + new],
        scratch_shapes=list(scratch) + ([pltpu.VMEM(ins[k].shape, ins[k].dtype) for k in held] + [pltpu.SemaphoreType.DMA((len(held),))] if held else []) + ([pltpu.SemaphoreType.DMA((total,)), pltpu.SemaphoreType.DMA((total,))] if total else []),
        input_output_aliases=al,
        compiler_params=pltpu.CompilerParams(vmem_limit_bytes=62 << 20, **(dict(collective_id=cid, has_side_effects=True) if total else {})),
        cost_estimate=pl.CostEstimate(flops=flops, bytes_accessed=nbytes, transcendentals=0),
        name=name)(*ins, *[locs[n] for n in lnames], *[bufs[g.name] for g in old])
    for g, b in zip(old + new, res[n_out:]):
        bufs[g.name] = b
    return res[:n_out]


GROWS = 16


def norm_body(nblk, skip, cin, couts, sc):
    x_ref, gl_ref = cin
    h_ref, gm_ref = couts
    gbuf, ga, ssem, rsem, osem = sc
    step = pl.program_id(0)
    me, dp = lax.axis_index("fsdp"), lax.axis_index("dp")
    mine = gbuf.at[pl.ds(pl.multiple_of(me * GROWS, GROWS), GROWS), :]
    sends = [pltpu.make_async_remote_copy(src_ref=gl_ref, dst_ref=mine, send_sem=ssem.at[j - 1], recv_sem=rsem.at[j - 1],
                                          device_id=(dp, lax.rem(me + j, nblk)), device_id_type=MESH) for j in range(1, nblk)]
    own = pltpu.make_async_copy(gl_ref, mine, osem.at[0])

    @pl.when(step == 0)
    def _():
        own.start()
        for cp in sends:
            cp.start()

    row = lambda k: jnp.concatenate([gbuf[b * GROWS + k:b * GROWS + k + 1, :] for b in range(nblk)], axis=1)

    @pl.when(step == skip)
    def _():
        own.wait()
        for cp in sends:
            cp.wait()
        gm_ref[...] = row(1)
        ga[...] = row(0).astype(F32)

    @pl.when(jnp.logical_and(step >= skip, step < pl.num_programs(0) - 1))
    def _():
        def rows(k, _):
            rs = pl.ds(pl.multiple_of(k * GROWS, GROWS), GROWS)
            x = x_ref[rs, :].astype(F32)
            r = lax.rsqrt(jnp.mean(x * x, axis=-1, keepdims=True) + EPS)
            h_ref[rs, :] = (x * r * ga[...]).astype(BF)
            return 0
        lax.fori_loop(0, x_ref.shape[0] // GROWS, rows, 0, unroll=4)


def proj_body(roped, cin, couts, sc):
    h_ref, w_refs, (cos_ref, sin_ref) = cin[0], cin[1:1 + len(roped)], cin[1 + len(roped):3 + len(roped)]
    hd = 2 * cos_ref.shape[1]
    c = jnp.concatenate([cos_ref[...], cos_ref[...]], axis=1)
    s = jnp.concatenate([-sin_ref[...], sin_ref[...]], axis=1)
    for w_ref, out_ref, rope in zip(w_refs, couts, roped):
        for n0 in range(0, w_ref.shape[1], 2 * hd):
            acc = jnp.dot(h_ref[...], w_ref[:, n0:n0 + 2 * hd], preferred_element_type=F32).astype(BF)
            for j in (0, hd):
                part = acc[:, j:j + hd]
                if rope:
                    t = part.astype(F32)
                    part = (t * c + pltpu.roll(t, hd // 2, 1) * s).astype(BF)
                out_ref[:, n0 + j:n0 + j + hd] = part


def attn_body(hd, qb, unroll, cin, couts, sc):
    q_ref, k_ref, v_ref = cin[:3]
    o_ref = couts[0]

    @pl.when(pl.program_id(0) == 0)
    def _():
        for src, dst in zip(cin[3:], couts[1:]):
            for j in range(dst.shape[1]):
                dst[:, j, :] = src[:, j * hd:(j + 1) * hd]
    S, nh = q_ref.shape[0], q_ref.shape[1] // hd
    scale = hd ** -0.5 * math.log2(math.e)
    mask = lax.broadcasted_iota(jnp.int32, (qb, qb), 0) >= lax.broadcasted_iota(jnp.int32, (qb, qb), 1)

    for b in range(S // qb):
        r0, n = b * qb, (b + 1) * qb

        def step(i, _):
            heads = [pl.ds(pl.multiple_of((i * unroll + u) * hd, hd), hd) for u in range(unroll)]
            scores = [lax.dot_general(q_ref[r0:n, hs], k_ref[:n, :], (((1,), (1,)), ((), ())), preferred_element_type=F32) for hs in heads]
            for hs, s in zip(heads, scores):
                diag = jnp.where(mask, s[:, r0:], -jnp.inf)
                s = diag if r0 == 0 else jnp.concatenate([s[:, :r0], diag], axis=1)
                p = jnp.exp2((s - jnp.max(s, axis=1, keepdims=True)) * scale)
                pb = (p * (1.0 / jnp.sum(p, axis=1, keepdims=True))).astype(BF)
                o_ref[r0:n, hs] = jnp.dot(pb, v_ref[:n, :], preferred_element_type=F32).astype(BF)
            return 0
        lax.fori_loop(0, nh // unroll, step, 0)


def wout_body(cin, couts, sc):
    o_ref, w_ref, x_ref, g_ref = cin
    x1_ref, h_ref = couts
    D = w_ref.shape[1]
    o = o_ref[...]
    ss = jnp.zeros((o.shape[0], 1), F32)
    step = min(512, D)
    for n0 in range(0, D, step):
        cs = slice(n0, n0 + step)
        a = jnp.dot(o, w_ref[:, cs], preferred_element_type=F32).astype(BF)
        x1 = (x_ref[:, cs].astype(F32) + a.astype(F32)).astype(BF)
        x1_ref[:, cs] = x1
        xf = x1.astype(F32)
        ss = ss + jnp.sum(xf * xf, axis=1, keepdims=True)
    r = lax.rsqrt(ss / D + EPS)
    for n0 in range(0, D, step):
        cs = slice(n0, n0 + step)
        h_ref[:, cs] = (x1_ref[:, cs].astype(F32) * r * g_ref[:, cs].astype(F32)).astype(BF)


def gu_loads(mt, cin, sc):
    hbuf, sem = sc
    return [pltpu.make_async_copy(cin[0].at[pl.ds(k * mt, mt), :], hbuf.at[pl.ds(k * mt, mt), :], sem.at[k]) for k in range(hbuf.shape[0] // mt)]


def gu_pre(mt, step, cin, sc):
    @pl.when(step == 0)
    def _():
        for cp in gu_loads(mt, cin, sc):
            cp.start()


def gu_body(mt, cin, couts, sc):
    wg_ref, wu_ref = cin[1:3]
    r_ref, = couts
    hbuf = sc[0]

    def rows(k, _):
        rs = pl.ds(pl.multiple_of(k * mt, mt), mt)

        @pl.when(pl.program_id(0) == 0)
        def _():
            pltpu.make_async_copy(cin[0].at[rs, :], hbuf.at[rs, :], sc[1].at[k]).wait()
        hh = hbuf[rs, :]
        g = jnp.dot(hh, wg_ref[...], preferred_element_type=F32).astype(BF).astype(F32)
        u = jnp.dot(hh, wu_ref[...], preferred_element_type=F32).astype(BF).astype(F32)
        r_ref[rs, :] = ((g / (1.0 + jnp.exp(-g))) * u).astype(BF)
        return 0
    lax.fori_loop(0, hbuf.shape[0] // mt, rows, 0)


def down_tiles(c0, r_ref, w_ref, x_ref, out_ref):
    m = jnp.dot(r_ref[...], w_ref[...], preferred_element_type=F32).astype(BF)
    out_ref[:, c0:c0 + w_ref.shape[1]] = (x_ref[...].astype(F32) + m.astype(F32)).astype(BF)


def down_loop(c0, r_ref, w_ref, x_ref, out_ref):
    def tile(n, _):
        cs = pl.ds(pl.multiple_of(n * UNIT, UNIT), UNIT)
        m = jnp.dot(r_ref[...], w_ref[:, cs], preferred_element_type=F32).astype(BF)
        out_ref[:, pl.ds(pl.multiple_of(c0 + n * UNIT, UNIT), UNIT)] = (x_ref[:, cs].astype(F32) + m.astype(F32)).astype(BF)
        return 0
    lax.fori_loop(0, w_ref.shape[1] // UNIT, tile, 0)


def down_body(cin, couts, sc):
    down_tiles(0, *cin, couts[0])


def down_loop_body(cin, couts, sc):
    down_loop(0, *cin, couts[0])


def last_body(cin, couts, sc):
    r_ref, w_ref, x_ref, *parts = cin
    out_ref, = couts
    c0 = 0
    for p in parts:
        out_ref[:, c0:c0 + p.shape[1]] = p[...]
        c0 += p.shape[1]
    down_tiles(c0, r_ref, w_ref, x_ref, out_ref)


UNIT = 256
GU_UNITS = (6, 6, 6, 6, 6, 6, 7)
DOWN_COLS = (512, 512, 512, 512)


def thirds(cols, unit, frac=1 / 3):
    outer = int(cols // unit * frac + 0.5) * unit
    return outer, cols - 2 * outer


def local_layer(nblk, hidden, g_attn, w_query, w_key, w_value, w_out, g_mlp, w_gate, w_up, w_down, cos_tab, sin_tab):
    B, S, D = hidden.shape
    T = B * S
    hd = 2 * cos_tab.shape[1]
    qw, kw = w_query.shape[1], w_key.shape[1]
    ff = w_gate.shape[1]
    kv = kw // hd
    x = hidden.reshape(T, D)
    gl = jnp.pad(jnp.stack([g_attn, g_mlp]), ((0, GROWS - 2), (0, 0)))
    locs = dict(wq=w_query, wk=w_key, wv=w_value, wo=w_out, wg=w_gate, wu=w_up, wd=w_down)
    rw = w_query.shape[0]
    qk = qw + 2 * kw
    half = qw // 2
    Q0 = [Group("q0", "wq", 0, 0, half, rw, nblk), Group("k", "wk", 0, 0, kw, rw, nblk), Group("v", "wv", 0, 0, kw, rw, nblk)]
    Q1 = [Group("q1", "wq", half, 0, half, rw, nblk)]
    WO = Group("wo", "wo", 0, *thirds(D, 128), rw, nblk)
    G, c0 = [], 0
    for k, u in enumerate(GU_UNITS):
        G.append([Group("g%d" % k, "wg", c0, *thirds(u * UNIT, 128), rw, nblk), Group("u%d" % k, "wu", c0, *thirds(u * UNIT, 128), rw, nblk)])
        c0 += u * UNIT
    assert c0 == ff
    Dn, c0 = [], 0
    for k, w in enumerate(DOWN_COLS):
        Dn.append(Group("d%d" % k, "wd", c0, *thirds(w, 128), w_down.shape[0], nblk))
        c0 += w
    assert c0 == D
    seq = [[g] if isinstance(g, Group) else g for g in G + Dn]

    def acts(i, late, extra=(), more=()):
        now = [(gs, s) for gs, s in extra]
        for s in (3, 2, 1):
            now += [(gs, s) for j, gs in enumerate(seq) if j + 2 + s - 1 == i]
        first = [(g, s) for gs, s in now for g in gs]
        then = list(more) + [(g, 4) for g, s in first if s == 3 and n_copies(g, 4)]
        return ([(0, first)] if first else []) + ([(late, then)] if then else [])

    bufs = {}
    run = functools.partial(call, bufs=bufs, locs=locs, nblk=nblk)
    sd = jax.ShapeDtypeStruct
    mt = 256
    row = lambda i: (i, 0)
    const = lambda *a: (0, 0)
    cid = 0
    skip, nrow = 1, T // mt
    last = nrow + skip - 1
    on = lambda gs, st: [(g, st) for g in gs if n_copies(g, st)]
    dma = pltpu.SemaphoreType.DMA
    rowk = lambda i: (jnp.clip(i - skip, 0, nrow - 1), 0)
    h, gm = run("gather_norm", cid, functools.partial(norm_body, nblk, skip), (nrow + skip + 1,), [x, gl],
                [pl.BlockSpec((mt, D), rowk), pl.BlockSpec(memory_space=HBM)],
                [sd((T, D), BF), sd((1, D), BF)], [pl.BlockSpec((mt, D), rowk), pl.BlockSpec((1, D), const)],
                [(0, on(Q0, 1)), (skip, on(Q0, 2) + on(Q1, 1)), (last + 1, on(Q0, 3))],
                scratch=[pltpu.VMEM((nblk * GROWS, gl.shape[1]), BF), pltpu.VMEM((1, D), F32), dma((nblk - 1,)), dma((nblk - 1,)), dma((1,))], everyone=True)
    tab = pl.BlockSpec((mt, hd // 2), lambda i: (i % (S // mt), 0))
    gw = qw // kv
    nt = T // mt
    wspec = lambda n: pl.BlockSpec((D, n), const)
    late = nt * 2 // 3

    def project(name, slot, ws, outs, specs, roped, extra, more=(), into=()):
        width = sum(bufs[w].shape[1] for w in ws)
        return run(name, cid, functools.partial(proj_body, roped), (nt,), [h] + [bufs[w] for w in ws] + [cos_tab, sin_tab] + list(into),
                   [pl.BlockSpec((mt, D), row)] + [wspec(bufs[w].shape[1]) for w in ws] + [tab, tab] + [pl.BlockSpec(memory_space=HBM)] * len(into),
                   outs, specs, acts(slot, late, extra, more), flops=2 * T * D * width, nbytes=4 * T * D,
                   held=tuple(range(1, 1 + len(ws))), alias={3 + len(ws): 0} if into else None)

    cid += 1
    q, k, v = project("proj0", 0, ["q0", "k", "v"], [sd((T, qw), BF), sd((T, kw), BF), sd((T, kw), BF)],
                      [pl.BlockSpec((mt, half), row), pl.BlockSpec((mt, kw), row), pl.BlockSpec((mt, kw), row)], (True, True, False),
                      [(Q1, 2), ([WO], 1)], [(Q1[0], 3)])
    cid += 1
    q, = project("proj1", 1, ["q1"], [sd((T, qw), BF)], [pl.BlockSpec((mt, half), lambda i: (i, 1))], (True,), [([WO], 2)], into=[q])
    cid += 1
    one = pl.BlockSpec((S, hd), lambda j, b: (b, j))
    grp = pl.BlockSpec((S, gw), lambda j, b: (b, j))
    whole = pl.BlockSpec((S, kw), lambda j, b: (jnp.where(j == 0, b, B - 1), 0))
    cube = pl.BlockSpec((S, kv, hd), lambda j, b: (jnp.where(j == 0, b, B - 1), 0, 0))
    ahead = [a for a in acts(3, 0)[0][1] if a[1] == 1]
    o, kc, vc = run("attn", cid, functools.partial(attn_body, hd, 256, 2), (kv, B), [q, k, v, k, v], [grp, one, one, whole, whole],
                    [sd((T, qw), BF)] + [sd((T, kv, hd), BF)] * 2, [grp, cube, cube],
                    [(0, acts(2, 0, [([WO], 3)])[0][1] + ahead), (kv * B // 2, [a for a in acts(3, 0)[0][1] if a not in ahead] + [(WO, 4)])], flops=T * S * qw * 8, nbytes=4 * T * qw)
    cid += 1
    x1, h2 = run("wout", cid, wout_body, (nt,), [o, bufs["wo"], x, gm],
                 [pl.BlockSpec((mt, qw), row), pl.BlockSpec((qw, D), const), pl.BlockSpec((mt, D), row), pl.BlockSpec((1, D), const)],
                 [sd((T, D), BF)] * 2, [pl.BlockSpec((mt, D), row)] * 2, acts(4, late), flops=2 * T * D * qw, nbytes=8 * T * D, held=(1,))
    r, n0 = None, 0
    mtg = S
    for j, u in enumerate(GU_UNITS):
        cid += 1
        hb = pl.BlockSpec(memory_space=HBM)
        ins = [h2, bufs["g%d" % j], bufs["u%d" % j]] + ([r] if r is not None else [])
        specs = [hb, pl.BlockSpec((D, UNIT), lambda n: (0, n)), pl.BlockSpec((D, UNIT), lambda n: (0, n))] + ([hb] if r is not None else [])
        r, = run("gateup%d" % j, cid, functools.partial(gu_body, mtg), (u,), ins, specs,
                 [sd((T, ff), BF)], [pl.BlockSpec((T, UNIT), lambda n, n0=n0: (0, n0 + n))],
                 acts(5 + j, u * 2 // 3), flops=4 * T * D * UNIT * u, nbytes=4 * T * D, alias={3: 0} if r is not None else None,
                 scratch=[pltpu.VMEM((T, D), BF), dma((T // mtg,))], pre=functools.partial(gu_pre, mtg))
        n0 += u
    parts, c0 = [], 0
    for j, w in enumerate(DOWN_COLS):
        cid += 1
        off = c0 // w
        ins = [r, bufs["d%d" % j], x1]
        specs = [pl.BlockSpec((mt, ff), row), pl.BlockSpec((ff, w), const), pl.BlockSpec((mt, w), lambda i, off=off: (i, off))]
        a = acts(5 + len(GU_UNITS) + j, late)
        cost = dict(flops=2 * T * ff * w, nbytes=2 * T * ff, held=(1,))
        if j < len(DOWN_COLS) - 1:
            parts += run("down%d" % j, cid, down_loop_body if j == 0 else down_body, (T // mt,), ins, specs, [sd((T, w), BF)], [pl.BlockSpec((mt, w), row)], a, **cost)
        else:
            assert not a
            out, = run("down%d" % j, cid, last_body, (T // mt,), ins + parts, specs + [pl.BlockSpec((mt, p.shape[1]), row) for p in parts],
                       [sd((T, D), BF)], [pl.BlockSpec((mt, D), row)], [], **cost)
        c0 += w
    return out.reshape(B, S, D), kc.reshape(B, S, kv, hd), vc.reshape(B, S, kv, hd)


def solution(mesh):
    tok = P(("dp", "fsdp"), None, None)
    cache = P(("dp", "fsdp"), None, None, None)
    rowp, gain, table = P("fsdp", None), P("fsdp"), P(None, None)
    return jax.shard_map(functools.partial(local_layer, mesh.shape["fsdp"]), mesh=mesh,
                         in_specs=(tok, gain, rowp, rowp, rowp, rowp, gain, rowp, rowp, rowp, table, table),
                         out_specs=(tok, cache, cache), check_vma=False)
```
